32 devices in a mesh: groups: 2 (over x), tm: 4 (over y, core), rows: 4 (over z).
Axes of the slice: x: 2, y: 2, z: 4, core: 2. Of those that a mesh axis runs over, the one named last changes fastest.
Arguments:
- features: bfloat16 [16, 8, 96, 512], P(('groups', 'tm'), 'rows'), parts along dimension 0, may hold values from -6 to 6
- spatial_weight: bfloat16 [3, 3, 512, 512], replicated, may hold values from -0.09375 to 0.09375
- temporal_weight: bfloat16 [3, 512, 512], replicated, may hold values from -0.15625 to 0.15625
- head_weight: bfloat16 [512, 16], replicated, may hold values from -0.25 to 0.25
- embed_weight: bfloat16 [64, 5120], replicated, may hold values from -0.75 to 0.75
- ada_scale: bfloat16 [5120], replicated, may hold values from -0.5 to 0.5
- ada_shift: bfloat16 [5120], replicated, may hold values from -3 to 3
- qkv_weight: bfloat16 [5120, 9216], P('tm', 'rows'), may hold values from -0.078125 to 0.078125
Outputs:
- qkv: float32 [3072, 9216], P(('groups', 'tm'), 'rows'), parts along dimension 0
The draws below stay inside these ranges and needn't reach their ends.
There are 2 independent parts, one for each index of `groups`. The reference program is written for one: setup_inputs(seed, part) draws one part's arguments, and reference() takes and returns one part's arrays. A program takes and returns all parts, laid end to end along the dimension named above; an argument that names none is the same for every part. Nothing has to cross between parts.
All inputs are finite; a program needn't handle non-finite values.
Results may differ from the reference program's by a relative error of at most 0.0056.
Values may be sent and summed in bfloat16 or wider, within the bound.
A program may use at most 128 MiB of HBM per device.

```python
import jax
import jax.numpy as jnp
from jax import lax

D = 5120
LATENT = 16
PATCH = 2
CH = 512
WIDTH = 96
FRAMES = 8
HEIGHT = 8
QKV = 9216
PDIM = 64
TOKENS = 1536


def block_levels(stream_key, dims, split, least, largest):
    def one(dim, shards_of):
        heights = jax.random.uniform(jax.random.fold_in(jax.random.fold_in(stream_key, 6), dim), (shards_of,), jnp.float32, least / len(split), largest / len(split))
        return jnp.repeat(jnp.exp(heights), dims[dim] // shards_of).reshape((-1,) + (1,) * (len(dims) - dim - 1))

    level = one(*split[0])
    for cut in split[1:]:
        level = level * one(*cut)
    return level


def scatter_about(own_key, dims, scale, limit, shards=(), held_as=jnp.bfloat16):
    values = scale * jax.random.normal(own_key, dims, jnp.float32)
    if shards:
        values = values * block_levels(own_key, dims, shards, -0.22, 0.18)
    return jnp.clip(values, -limit, limit).astype(held_as)


def setup_inputs(seed: int = 0, part: int = 0) -> dict:
    arg_keys = jax.random.split(jax.random.key(seed), 9)
    part_splits = jax.random.split(jax.random.fold_in(arg_keys[8], part), 9)
    return {
        "features": scatter_about(part_splits[0], (FRAMES, HEIGHT, WIDTH, CH), 1.0, 6.0, ((0, 4), (1, 4))),
        "spatial_weight": scatter_about(arg_keys[1], (3, 3, CH, CH), (9 * CH) ** -0.5, 0.09375),
        "temporal_weight": scatter_about(arg_keys[2], (3, CH, CH), (3 * CH) ** -0.5, 0.15625),
        "head_weight": scatter_about(arg_keys[3], (CH, LATENT), CH ** -0.5, 0.25),
        "embed_weight": scatter_about(arg_keys[4], (PDIM, D), PDIM ** -0.5, 0.75),
        "ada_scale": jnp.clip(jax.random.uniform(arg_keys[5], (D,), jnp.float32, -0.5, 0.5), -0.5, 0.5).astype(jnp.bfloat16),
        "ada_shift": scatter_about(arg_keys[6], (D,), 0.5, 3.0),
        "qkv_weight": scatter_about(arg_keys[7], (D, QKV), D ** -0.5, 0.078125, ((0, 4), (1, 4))),
    }


def norm_silu(values):
    scaled = values * jax.lax.rsqrt(lax.optimization_barrier(jnp.mean(values * values, axis=-1, keepdims=True)) + 1e-06)
    return jax.nn.silu(scaled)

def reference(features, spatial_weight, temporal_weight, head_weight, embed_weight, ada_scale, ada_shift, qkv_weight):
    activated = norm_silu(features.astype(jnp.float32)).astype(jnp.bfloat16)
    padded = jnp.pad(activated, ((0, 0), (1, 1), (1, 1), (0, 0)))
    spatial = jnp.zeros((FRAMES * HEIGHT * WIDTH, CH), jnp.float32)
    for tap_row in range(3):
        for tap_col in range(3):
            window = padded[:, tap_row:tap_row + HEIGHT, tap_col:tap_col + WIDTH].reshape(-1, CH)
            spatial = spatial + jnp.dot(window, spatial_weight[tap_row, tap_col], preferred_element_type=jnp.float32)
    mixed_act = norm_silu(spatial).astype(jnp.bfloat16).reshape(FRAMES, HEIGHT, WIDTH, CH)
    stacked = jnp.pad(mixed_act, ((2, 0), (0, 0), (0, 0), (0, 0)))
    temporal = jnp.zeros((FRAMES * HEIGHT * WIDTH, CH), jnp.float32)
    for tap in range(3):
        temporal = temporal + jnp.dot(stacked[tap:tap + FRAMES].reshape(-1, CH), temporal_weight[tap], preferred_element_type=jnp.float32)
    summed = features.astype(jnp.float32).reshape(-1, CH) + temporal
    latent = jnp.dot(norm_silu(summed).astype(jnp.bfloat16), head_weight, preferred_element_type=jnp.float32).astype(jnp.bfloat16)
    latent = latent.reshape(FRAMES, HEIGHT // PATCH, PATCH, WIDTH // PATCH, PATCH, LATENT)
    patches = jnp.transpose(latent, (0, 1, 3, 2, 4, 5)).reshape(TOKENS, PDIM)
    embedded = jnp.dot(patches, embed_weight, preferred_element_type=jnp.float32).astype(jnp.bfloat16)
    widened = lax.optimization_barrier(embedded).astype(jnp.float32)
    centered = widened - lax.optimization_barrier(jnp.mean(widened, axis=-1, keepdims=True))
    spread = lax.optimization_barrier(jnp.mean(centered * centered, axis=-1, keepdims=True))
    modulated = centered * lax.rsqrt(spread + 1e-06) * (1.0 + ada_scale.astype(jnp.float32)) + ada_shift.astype(jnp.float32)
    normalized = modulated.astype(jnp.bfloat16)
    return jnp.dot(normalized, qkv_weight, preferred_element_type=jnp.float32)
```

```python
import jax
import jax.numpy as jnp
from jax import lax
from jax.sharding import PartitionSpec as P

LATENT = 16
PATCH = 2
PDIM = 64


def with_halo(cells, sides, width):
    for axis, dim in sides:
        count = lax.axis_size(axis)
        ends = count - 1
        head = lax.slice_in_dim(cells, 0, width, axis=dim)
        tail = lax.slice_in_dim(cells, cells.shape[dim] - width, cells.shape[dim], axis=dim)
        cells = jnp.concatenate(
            [
                lax.ppermute(tail, axis, [(i, (i + 1) % count) for i in range(ends)]),
                cells,
                lax.ppermute(head, axis, [((i + 1) % count, i) for i in range(ends)]),
            ],
            axis=dim,
        )
    return cells


def passed_along(block, axis, distance):
    devices = range(lax.axis_size(axis))
    route = [(i - distance, i) for i in devices if i - distance in devices]
    return lax.ppermute(block, axis, route)


def halves(values):
    high = lax.reduce_precision(values, 8, 7)
    return high.astype(jnp.bfloat16), (values - high).astype(jnp.bfloat16)


def summed_over(values, axis):
    count = lax.axis_size(axis)
    if count & (count - 1):
        return lax.psum(values, axis)
    step = 1
    while step < count:
        values = values + lax.ppermute(values, axis, [(i, i ^ step) for i in range(count)])
        step *= 2
    return values


def norm_silu(values):
    scaled = values * lax.rsqrt(jnp.mean(values * values, axis=-1, keepdims=True) + 1e-06)
    return jax.nn.silu(scaled)


def per_device(
    features,
    spatial_weight,
    temporal_weight,
    head_weight,
    embed_weight,
    ada_scale,
    ada_shift,
    qkv_weight,
):
    frames_dev, rows_dev, columns, channels = features.shape
    depth = qkv_weight.shape[0]
    start = lax.axis_index("tm") * depth
    wide = embed_weight.astype(jnp.float32)
    wide = wide - jnp.mean(wide, axis=1, keepdims=True)
    gram = lax.dot_general(
        wide, wide, (((1,), (1,)), ((), ())), precision=lax.Precision.HIGHEST
    ) / wide.shape[1]
    scaled = lax.dynamic_slice_in_dim(
        wide * (1.0 + ada_scale.astype(jnp.float32)), start, depth, axis=1
    )
    shift = lax.dynamic_slice_in_dim(ada_shift, start, depth, axis=0)
    terms = jnp.dot(
        jnp.concatenate([*halves(scaled), shift[None]], axis=0),
        qkv_weight,
        preferred_element_type=jnp.float32,
    )
    folded = summed_over(
        jnp.concatenate([terms[:PDIM] + terms[PDIM : 2 * PDIM], terms[2 * PDIM :]], axis=0), "tm"
    )
    activated = norm_silu(features.astype(jnp.float32)).astype(jnp.bfloat16)
    rimmed = with_halo(activated, (("rows", 1),), 1)
    padded = jnp.pad(rimmed, ((0, 0), (0, 0), (1, 1), (0, 0)))
    spatial = jnp.zeros((frames_dev * rows_dev * columns, channels), jnp.float32)
    for tap_row in range(3):
        for tap_col in range(3):
            window = padded[:, tap_row : tap_row + rows_dev, tap_col : tap_col + columns].reshape(
                -1, channels
            )
            spatial = spatial + jnp.dot(
                window, spatial_weight[tap_row, tap_col], preferred_element_type=jnp.float32
            )
    mixed_act = (
        norm_silu(spatial).astype(jnp.bfloat16).reshape(frames_dev, rows_dev, columns, channels)
    )
    before = passed_along(mixed_act, "tm", 1)
    stacked = jnp.concatenate([before, mixed_act], axis=0)
    temporal = jnp.zeros((frames_dev * rows_dev * columns, channels), jnp.float32)
    for tap in range(3):
        temporal = temporal + jnp.dot(
            stacked[tap : tap + frames_dev].reshape(-1, channels),
            temporal_weight[tap],
            preferred_element_type=jnp.float32,
        )
    summed = features.astype(jnp.float32).reshape(-1, channels) + temporal
    latent = jnp.dot(
        norm_silu(summed).astype(jnp.bfloat16), head_weight, preferred_element_type=jnp.float32
    ).astype(jnp.bfloat16)
    latent = latent.reshape(frames_dev, 1, PATCH, columns // PATCH, PATCH, LATENT)
    patches = jnp.transpose(latent, (0, 1, 3, 2, 4, 5)).reshape(
        frames_dev, 1, columns // PATCH, PDIM
    )
    token_block = lax.all_gather(patches, "rows", axis=1, tiled=True)
    block_rows = token_block.shape[0] * token_block.shape[1] * token_block.shape[2]
    block = token_block.reshape(block_rows, PDIM)
    moment = jnp.dot(
        block.astype(jnp.float32), gram, precision=lax.Precision.HIGHEST
    ) * block.astype(jnp.float32)
    spread = jnp.maximum(jnp.sum(moment, axis=-1, keepdims=True), 0.0)
    product = jnp.dot(
        jnp.concatenate([block, block], axis=1),
        jnp.concatenate(halves(folded[:PDIM]), axis=0),
        preferred_element_type=jnp.float32,
    )
    projected = product * lax.rsqrt(spread + 1e-06) + folded[PDIM : PDIM + 1]
    return projected


def solution(mesh):
    return jax.shard_map(
        per_device,
        mesh=mesh,
        in_specs=(
            P(("groups", "tm"), "rows", None, None),
            P(),
            P(),
            P(),
            P(),
            P(),
            P(),
            P("tm", "rows"),
        ),
        out_specs=P(("groups", "tm"), "rows"),
        check_vma=False,
    )
```

```python
import functools

import jax
import jax.numpy as jnp
from jax import lax
from jax.experimental import pallas as pl
from jax.experimental.pallas import tpu as pltpu
from jax.sharding import PartitionSpec as P

LATENT = 16
PATCH = 2
PDIM = 64


def with_halo(cells, sides, width):
    for axis, dim in sides:
        count = lax.axis_size(axis)
        ends = count - 1
        head = lax.slice_in_dim(cells, 0, width, axis=dim)
        tail = lax.slice_in_dim(cells, cells.shape[dim] - width, cells.shape[dim], axis=dim)
        cells = jnp.concatenate(
            [
                lax.ppermute(tail, axis, [(i, (i + 1) % count) for i in range(ends)]),
                cells,
                lax.ppermute(head, axis, [((i + 1) % count, i) for i in range(ends)]),
            ],
            axis=dim,
        )
    return cells


def passed_along(block, axis, distance):
    devices = range(lax.axis_size(axis))
    route = [(i - distance, i) for i in devices if i - distance in devices]
    return lax.ppermute(block, axis, route)


def halves(values):
    high = lax.reduce_precision(values, 8, 7)
    return high.astype(jnp.bfloat16), (values - high).astype(jnp.bfloat16)


def paired_halves(values):
    count = lax.axis_size("tm")
    odd = lax.rem(lax.axis_index("tm"), 2) == 1
    width = values.shape[1] // 2
    low, high = values[:, :width], values[:, width:]
    beside = [(i, i ^ 1) for i in range(count)]
    return jnp.where(odd, high, low) + lax.ppermute(jnp.where(odd, low, high), "tm", beside)


def summed_over_pairs(kept):
    count = lax.axis_size("tm")
    step = 2
    while step < count:
        route = [(i, i ^ step) for i in range(count)]
        kept = kept + lax.ppermute(kept.astype(jnp.bfloat16), "tm", route).astype(jnp.float32)
        step *= 2
    return kept


def both_halves(kept):
    odd = lax.rem(lax.axis_index("tm"), 2) == 1
    other = lax.ppermute(kept, "tm", [(i, i ^ 1) for i in range(lax.axis_size("tm"))])
    return jnp.concatenate([jnp.where(odd, other, kept), jnp.where(odd, kept, other)], axis=1)


def gather_kernel(count, own_ref, out_ref, held, send_sem, recv_sem):
    me = lax.axis_index("rows")
    barrier = pltpu.get_barrier_semaphore()
    for hop in range(1, count):
        pl.semaphore_signal(
            barrier,
            inc=1,
            device_id={"rows": lax.rem(me + hop, count)},
            device_id_type=pl.DeviceIdType.MESH,
        )
    pl.semaphore_wait(barrier, count - 1)
    copies = []
    for hop in range(1, count):
        copy = pltpu.make_async_remote_copy(
            src_ref=own_ref,
            dst_ref=held.at[hop - 1],
            send_sem=send_sem.at[hop - 1],
            recv_sem=recv_sem.at[hop - 1],
            device_id={"rows": lax.rem(me + hop, count)},
            device_id_type=pl.DeviceIdType.MESH,
        )
        copy.start()
        copies.append(copy)
    out_ref[:, me] = own_ref[...]
    for hop in range(1, count):
        copies[hop - 1].wait()
        out_ref[:, lax.rem(me - hop + count, count)] = held[hop - 1]


def gathered(patches):
    count = lax.axis_size("rows")
    frames, tokens, entries = patches.shape
    return pl.pallas_call(
        functools.partial(gather_kernel, count),
        out_shape=jax.ShapeDtypeStruct((frames, count, tokens, entries), patches.dtype),
        in_specs=[pl.BlockSpec(memory_space=pltpu.VMEM)],
        out_specs=pl.BlockSpec(memory_space=pltpu.VMEM),
        scratch_shapes=[
            pltpu.VMEM((count - 1, frames, tokens, entries), patches.dtype),
            pltpu.SemaphoreType.DMA((count - 1,)),
            pltpu.SemaphoreType.DMA((count - 1,)),
        ],
        compiler_params=pltpu.CompilerParams(collective_id=0, has_side_effects=True),
        cost_estimate=pl.CostEstimate(flops=0, bytes_accessed=16_000_000, transcendentals=0),
    )(patches)


def norm_silu(values):
    scaled = values * lax.rsqrt(jnp.mean(values * values, axis=-1, keepdims=True) + 1e-06)
    return jax.nn.silu(scaled)


def per_device(
    features,
    spatial_weight,
    temporal_weight,
    head_weight,
    embed_weight,
    ada_scale,
    ada_shift,
    qkv_weight,
):
    frames_dev, rows_dev, columns, channels = features.shape
    activated = norm_silu(features.astype(jnp.float32)).astype(jnp.bfloat16)
    activated, embed_weight = lax.optimization_barrier((activated, embed_weight))
    depth = qkv_weight.shape[0]
    start = lax.axis_index("tm") * depth
    wide = embed_weight.astype(jnp.float32)
    wide = wide - jnp.mean(wide, axis=1, keepdims=True)
    gram = lax.dot_general(
        wide, wide, (((1,), (1,)), ((), ())), precision=lax.Precision.HIGHEST
    ) / wide.shape[1]
    scaled = lax.dynamic_slice_in_dim(
        wide * (1.0 + ada_scale.astype(jnp.float32)), start, depth, axis=1
    )
    shift = lax.dynamic_slice_in_dim(ada_shift, start, depth, axis=0)
    terms = jnp.dot(
        jnp.concatenate([*halves(scaled), shift[None]], axis=0),
        qkv_weight,
        preferred_element_type=jnp.float32,
    )
    kept = paired_halves(
        jnp.concatenate([terms[:PDIM] + terms[PDIM : 2 * PDIM], terms[2 * PDIM :]], axis=0)
    )
    rimmed = with_halo(activated, (("rows", 1),), 1)
    padded = jnp.pad(rimmed, ((0, 0), (0, 0), (1, 1), (0, 0)))
    padded, kept = lax.optimization_barrier((padded, kept))
    kept = summed_over_pairs(kept)
    spatial = jnp.zeros((frames_dev * rows_dev * columns, channels), jnp.float32)
    for tap_row in range(3):
        for tap_col in range(3):
            window = padded[:, tap_row : tap_row + rows_dev, tap_col : tap_col + columns].reshape(
                -1, channels
            )
            spatial = spatial + jnp.dot(
                window, spatial_weight[tap_row, tap_col], preferred_element_type=jnp.float32
            )
    mixed_act = (
        norm_silu(spatial).astype(jnp.bfloat16).reshape(frames_dev, rows_dev, columns, channels)
    )
    folded = both_halves(kept)
    before = passed_along(mixed_act, "tm", 1)
    stacked = jnp.concatenate([before, mixed_act], axis=0)
    temporal = jnp.zeros((frames_dev * rows_dev * columns, channels), jnp.float32)
    for tap in range(3):
        temporal = temporal + jnp.dot(
            stacked[tap : tap + frames_dev].reshape(-1, channels),
            temporal_weight[tap],
            preferred_element_type=jnp.float32,
        )
    summed = features.astype(jnp.float32).reshape(-1, channels) + temporal
    latent = jnp.dot(
        norm_silu(summed).astype(jnp.bfloat16), head_weight, preferred_element_type=jnp.float32
    ).astype(jnp.bfloat16)
    latent = latent.reshape(frames_dev, 1, PATCH, columns // PATCH, PATCH, LATENT)
    patches = jnp.transpose(latent, (0, 1, 3, 2, 4, 5)).reshape(
        frames_dev, columns // PATCH, PDIM
    )
    token_block = gathered(patches)
    block_rows = token_block.shape[0] * token_block.shape[1] * token_block.shape[2]
    block = token_block.reshape(block_rows, PDIM)
    moment = jnp.dot(
        block.astype(jnp.float32), gram, precision=lax.Precision.HIGHEST
    ) * block.astype(jnp.float32)
    spread = jnp.maximum(jnp.sum(moment, axis=-1, keepdims=True), 0.0)
    product = jnp.dot(
        jnp.concatenate([block, block], axis=1),
        jnp.concatenate(halves(folded[:PDIM]), axis=0),
        preferred_element_type=jnp.float32,
    )
    projected = product * lax.rsqrt(spread + 1e-06) + folded[PDIM : PDIM + 1]
    return projected


def solution(mesh):
    return jax.shard_map(
        per_device,
        mesh=mesh,
        in_specs=(
            P(("groups", "tm"), "rows", None, None),
            P(),
            P(),
            P(),
            P(),
            P(),
            P(),
            P("tm", "rows"),
        ),
        out_specs=P(("groups", "tm"), "rows"),
        check_vma=False,
    )
```
